32 devices in a mesh: rep: 1 (over z), row: 4 (over y), col: 4 (over x), core: 2 (over core).
Axes of the slice: x: 4, y: 4, z: 1, core: 2. Of those that a mesh axis runs over, the one named last changes fastest.
The devices are a block of a 4x4x8 slice.
Arguments:
- x: bfloat16 [2, 8192, 896], P(None, ('rep', 'row', 'col', 'core'))
- route_idx: int32 [2, 8192, 8], P(None, ('rep', 'row', 'col', 'core'))
- gates: float32 [2, 8192, 8], P(None, ('rep', 'row', 'col', 'core'))
- w_gate: bfloat16 [64, 896, 640], P(('rep', 'row', 'col', 'core'))
- w_up: bfloat16 [64, 896, 640], P(('rep', 'row', 'col', 'core'))
- w_down: bfloat16 [64, 640, 896], P(('rep', 'row', 'col', 'core'))
- grad_y: bfloat16 [2, 8192, 896], P(None, ('rep', 'row', 'col', 'core'))
Outputs:
- output 1: bfloat16 [2, 8192, 896], P(None, ('rep', 'row', 'col', 'core'))
- output 2: bfloat16 [2, 8192, 896], P(None, ('rep', 'row', 'col', 'core'))
- output 3: float32 [2, 8192, 8], P(None, ('rep', 'row', 'col', 'core'))
- output 4: float32 [64, 896, 640], P(('rep', 'row', 'col', 'core'))
- output 5: float32 [64, 896, 640], P(('rep', 'row', 'col', 'core'))
- output 6: float32 [64, 640, 896], P(('rep', 'row', 'col', 'core'))
All inputs are finite; a program needn't handle non-finite values.
Results may differ from the reference program's by a relative error of at most 0.0104298.
Values are sent between devices in bfloat16 or wider.
A program may use at most 768 MiB of HBM per device.

```python
import jax
import jax.numpy as jnp
from jax import lax

D_MODEL = 896
D_FF = 640
EXPERTS = 64
TOP_K = 8
TOK_DEV = 256
N_ROWS = 4
N_COLS = 4
N_CORES = 2

GROUP_SIZE = N_ROWS * N_COLS * N_CORES
TOKENS = GROUP_SIZE * TOK_DEV
CAPACITY = TOK_DEV // 2
CHIP_EXP = EXPERTS // (N_ROWS * N_COLS)
N_HOT = min(CHIP_EXP, TOP_K // 2)
N_COLD = EXPERTS - N_HOT
LOAD_MAX = GROUP_SIZE * CAPACITY


def draw_hot_chips(base_key):
    key_list = jax.random.split(base_key, 4)
    row_first = jax.random.randint(key_list[0], (), 0, N_ROWS)
    col_first = jax.random.randint(key_list[1], (), 0, N_COLS)
    row_second = (row_first + jax.random.randint(key_list[2], (), 1, N_ROWS)) % N_ROWS
    col_second = (col_first + jax.random.randint(key_list[3], (), 1, N_COLS)) % N_COLS
    return row_first * N_COLS + col_first, row_second * N_COLS + col_second


def draw_routing(base_key, hot_chip):
    key_list = jax.random.split(base_key, 4)
    slot_ids = jnp.arange(TOP_K)
    hot_ids = hot_chip * CHIP_EXP + jnp.arange(N_HOT) * (CHIP_EXP // N_HOT)
    sel_keys = jax.random.split(key_list[0], GROUP_SIZE * N_HOT)
    perm_rank = jax.vmap(lambda sub_key: jax.random.permutation(sub_key, TOK_DEV))(sel_keys)
    hot_mask = (perm_rank < CAPACITY).astype(jnp.int32).reshape(GROUP_SIZE, N_HOT, TOK_DEV)
    hot_mask = jnp.transpose(hot_mask, (0, 2, 1))
    hot_count = jnp.sum(hot_mask, axis=2)
    hot_rank = jnp.cumsum(hot_mask, axis=2) - hot_mask
    hot_pick = hot_mask[:, :, :, None] * (hot_rank[:, :, :, None] == slot_ids).astype(jnp.int32)
    hot_route = jnp.sum(hot_pick * hot_ids[None, None, :, None], axis=2)
    is_hot = jnp.zeros((EXPERTS,), jnp.int32).at[hot_ids].set(1)
    cold_sorted = jnp.argsort(is_hot * EXPERTS + jnp.arange(EXPERTS))[:N_COLD]
    cold_keys = jax.random.split(key_list[1], GROUP_SIZE)
    cold_perm = jax.vmap(lambda sub_key: jax.random.permutation(sub_key, cold_sorted))(cold_keys)
    win_start = jax.random.randint(key_list[2], (GROUP_SIZE, 1, 1), 0, N_COLD)
    cold_offset = slot_ids[None, None, :] - hot_count[:, :, None]
    cold_pos = (win_start + jnp.arange(TOK_DEV)[None, :, None] * TOP_K + cold_offset) % N_COLD
    cold_route = jnp.take_along_axis(cold_perm, cold_pos.reshape(GROUP_SIZE, TOK_DEV * TOP_K), axis=1)
    route_ids = jnp.where(cold_offset < 0, hot_route, cold_route.reshape(GROUP_SIZE, TOK_DEV, TOP_K))
    slot_rot = jax.random.randint(key_list[3], (GROUP_SIZE, TOK_DEV, 1), 0, TOP_K)
    route_ids = jnp.take_along_axis(route_ids, (slot_ids - slot_rot) % TOP_K, axis=2)
    return route_ids.reshape(TOKENS, TOP_K).astype(jnp.int32)


def setup_inputs(seed: int = 0, part: int = 0) -> dict:
    base_key = jax.random.fold_in(jax.random.key(seed), part)
    key_list = jax.random.split(base_key, 9)
    hot_first, hot_second = draw_hot_chips(key_list[0])
    route_idx = jnp.stack([draw_routing(key_list[1], hot_first), draw_routing(key_list[2], hot_second)])
    x = jax.random.normal(key_list[3], (2, TOKENS, D_MODEL), jnp.float32).astype(jnp.bfloat16)
    raw_gates = jax.random.uniform(key_list[4], (2, TOKENS, TOP_K), jnp.float32, 1.0, 2.0)
    gates = raw_gates / jnp.sum(raw_gates, axis=2, keepdims=True)
    w_gate = (jax.random.normal(key_list[5], (EXPERTS, D_MODEL, D_FF), jnp.float32) * D_MODEL ** -0.5).astype(jnp.bfloat16)
    w_up = (jax.random.normal(key_list[6], (EXPERTS, D_MODEL, D_FF), jnp.float32) * D_MODEL ** -0.5).astype(jnp.bfloat16)
    w_down = (jax.random.normal(key_list[7], (EXPERTS, D_FF, D_MODEL), jnp.float32) * D_FF ** -0.5).astype(jnp.bfloat16)
    grad_y = jax.random.normal(key_list[8], (2, TOKENS, D_MODEL), jnp.float32).astype(jnp.bfloat16)
    return {"x": x, "route_idx": route_idx, "gates": gates, "w_gate": w_gate, "w_up": w_up, "w_down": w_down, "grad_y": grad_y}


def swiglu_rows(x_rows, d_out, w_gate_e, w_up_e, w_down_e):
    gate_pre = jnp.dot(x_rows, w_gate_e, preferred_element_type=jnp.float32).astype(jnp.bfloat16)
    up_pre = jnp.dot(x_rows, w_up_e, preferred_element_type=jnp.float32).astype(jnp.bfloat16)
    gate_f = gate_pre.astype(jnp.float32)
    up_f = up_pre.astype(jnp.float32)
    sigmoid_g = jax.nn.sigmoid(gate_f)
    hidden = (gate_f * sigmoid_g * up_f).astype(jnp.bfloat16)
    exp_out = jnp.dot(hidden, w_down_e, preferred_element_type=jnp.float32).astype(jnp.bfloat16)
    d_act = jnp.dot(d_out, w_down_e.T, preferred_element_type=jnp.float32)
    d_up = (d_act * gate_f * sigmoid_g).astype(jnp.bfloat16)
    d_gate = (d_act * up_f * sigmoid_g * (1.0 + gate_f * (1.0 - sigmoid_g))).astype(jnp.bfloat16)
    d_in = (jnp.dot(d_gate, w_gate_e.T, preferred_element_type=jnp.float32) + jnp.dot(d_up, w_up_e.T, preferred_element_type=jnp.float32)).astype(jnp.bfloat16)
    g_gate = jnp.dot(x_rows.T, d_gate, preferred_element_type=jnp.float32)
    g_up = jnp.dot(x_rows.T, d_up, preferred_element_type=jnp.float32)
    g_down = jnp.dot(hidden.T, d_out, preferred_element_type=jnp.float32)
    return exp_out, d_in, g_gate, g_up, g_down


def microbatch(x, route_ids, gates, grad_y, w_gate, w_up, w_down):
    token_ids = jnp.arange(TOKENS)
    member = jnp.zeros((TOKENS, EXPERTS), jnp.int32).at[token_ids[:, None], route_ids].set(1)
    slot_rank = jnp.cumsum(member, axis=0) - member
    slot_pos = jnp.take_along_axis(slot_rank, route_ids, axis=1)
    slot_owner = jnp.full((EXPERTS * LOAD_MAX,), TOKENS * TOP_K, jnp.int32)
    slot_owner = slot_owner.at[(route_ids * LOAD_MAX + slot_pos).reshape(-1)].set(jnp.arange(TOKENS * TOP_K))
    slot_owner = slot_owner.reshape(EXPERTS, LOAD_MAX)
    x_pad = jnp.concatenate([x, jnp.zeros((1, D_MODEL), x.dtype)])
    dy_pad = jnp.concatenate([grad_y, jnp.zeros((1, D_MODEL), grad_y.dtype)])
    gate_pad = jnp.concatenate([gates.reshape(-1), jnp.zeros((1,), jnp.float32)])

    def one_expert(accums, per_expert):
        y_acc, dx_acc, dg_acc = accums
        slot_ids, w_gate_e, w_up_e, w_down_e = per_expert
        tok_rows = slot_ids // TOP_K
        row_gate = gate_pad[slot_ids]
        x_rows = x_pad[tok_rows]
        dy_rows = dy_pad[tok_rows].astype(jnp.float32)
        d_out = (row_gate[:, None] * dy_rows).astype(jnp.bfloat16)
        exp_out, d_in, g_gate, g_up, g_down = swiglu_rows(x_rows, d_out, w_gate_e, w_up_e, w_down_e)
        out_f = exp_out.astype(jnp.float32)
        y_acc = y_acc.at[tok_rows].add(row_gate[:, None] * out_f)
        dx_acc = dx_acc.at[tok_rows].add(d_in.astype(jnp.float32))
        dg_acc = dg_acc.at[slot_ids].add(jnp.sum(dy_rows * out_f, axis=1))
        return (y_acc, dx_acc, dg_acc), (g_gate, g_up, g_down)

    init_acc = (jnp.zeros((TOKENS + 1, D_MODEL), jnp.float32), jnp.zeros((TOKENS + 1, D_MODEL), jnp.float32), jnp.zeros((TOKENS * TOP_K + 1,), jnp.float32))
    final_acc, grads = lax.scan(one_expert, init_acc, (slot_owner, w_gate, w_up, w_down))
    y_acc, dx_acc, dg_acc = final_acc
    y_out = y_acc[:TOKENS].astype(jnp.bfloat16)
    dx_out = dx_acc[:TOKENS].astype(jnp.bfloat16)
    dg_out = dg_acc[:TOKENS * TOP_K].reshape(TOKENS, TOP_K)
    return y_out, dx_out, dg_out, grads[0], grads[1], grads[2]


def reference(x, route_idx, gates, w_gate, w_up, w_down, grad_y):
    mb_first = microbatch(x[0], route_idx[0], gates[0], grad_y[0], w_gate, w_up, w_down)
    mb_second = microbatch(x[1], route_idx[1], gates[1], grad_y[1], w_gate, w_up, w_down)
    return (jnp.stack([mb_first[0], mb_second[0]]), jnp.stack([mb_first[1], mb_second[1]]), jnp.stack([mb_first[2], mb_second[2]]), mb_first[3] + mb_second[3], mb_first[4] + mb_second[4], mb_first[5] + mb_second[5])
```

```python
import functools

import jax
import jax.numpy as jnp
from jax import lax
from jax.experimental import pallas as pl
from jax.experimental.pallas import tpu as pltpu
from jax.sharding import PartitionSpec as P

GROUP_AXES = ("row", "col", "core")
ALL_AXES = ("rep", "row", "col", "core")
TILE = 256
LANES = 128


def expert_kernel(dims, first, *refs):
    nblk, span, tok, model, ff, experts, cap = dims
    nsup = nblk // span
    seg, last_row, tiles, pos_rows, tokens, cols_hbm, wgu_hbm, wd_hbm, wdt_hbm, wgut_hbm = refs[:10]
    refs = refs[10:]
    if not first:
        prev, refs = refs[:3], refs[3:]
    out_hbm, dg_hbm, gg_hbm, gu_hbm, gd_hbm = refs[:5]
    (rows_x, rows_q, wgu, wd, wdt, wgut, acc_gu, acc_d, xbuf, dybuf, colbuf, outbuf, dgbuf, dh, sem_x, sem_dy, sem_c,
     sem_w, sem_a, sem_out, sem_dg) = refs[5:]

    def x_copy(s):
        return pltpu.make_async_copy(tokens.at[0, pl.ds(s * span * tok, span * tok)], xbuf, sem_x)

    def dy_copy(s, slot):
        return pltpu.make_async_copy(tokens.at[1, pl.ds(s * span * tok, span * tok)], dybuf.at[slot], sem_dy.at[slot])

    def col_copy(s, slot):
        return pltpu.make_async_copy(cols_hbm.at[pl.ds(s * span * tok, span * tok)], colbuf.at[slot], sem_c.at[slot])

    def out_copies(blk, slot):
        where = pl.ds(blk * tok, tok)
        return (pltpu.make_async_copy(outbuf.at[slot], out_hbm.at[where], sem_out.at[slot]),
                pltpu.make_async_copy(dgbuf.at[slot], dg_hbm.at[where], sem_dg.at[slot]))

    weights = [pltpu.make_async_copy(src, dst, sem_w.at[i])
               for i, (src, dst) in enumerate(((wgu_hbm, wgu), (wd_hbm, wd), (wdt_hbm, wdt), (wgut_hbm, wgut)))]
    sums = (acc_gu.at[:, :, pl.ds(0, ff)], acc_gu.at[:, :, pl.ds(ff, ff)], acc_d)

    x_copy(0).start()
    dy_copy(0, 0).start()
    col_copy(0, 0).start()
    for copy in weights:
        copy.start()
    if first:
        for e in range(experts):
            @pl.loop(0, model // 128)
            def _(i, e=e):
                acc_gu[e, pl.ds(i * 128, 128), :] = jnp.zeros((128, 2 * ff), jnp.float32)

            @pl.loop(0, ff // 128)
            def _(i, e=e):
                acc_d[e, pl.ds(i * 128, 128), :] = jnp.zeros((128, model), jnp.float32)
    else:
        for i, (src, dst) in enumerate(zip(prev, sums)):
            pltpu.make_async_copy(src, dst, sem_a.at[i]).start()

    def step(s, carry):
        slot = lax.rem(s, 2)
        x_copy(s).wait()
        dy_copy(s, slot).wait()
        col_copy(s, slot).wait()

        @pl.when(s + 1 < nsup)
        def _():
            dy_copy(s + 1, 1 - slot).start()
            col_copy(s + 1, 1 - slot).start()

        def pack(b, carry):
            rows = pl.ds(pl.multiple_of(b * tok, tok), tok)
            blk = s * span + b
            x_b = xbuf[rows, :]
            dy_b = dybuf[slot, rows, :].astype(jnp.float32)
            for e in range(experts):
                gate = colbuf[slot, rows, e:e + 1]
                q_b = (gate * dy_b).astype(jnp.bfloat16)
                hit = lax.broadcasted_iota(jnp.int32, (cap, tok), 0) == pos_rows[e, pl.ds(blk, 1), :]
                pick = jnp.where(hit, 1.0, 0.0).astype(jnp.bfloat16)
                at = pl.ds(pl.multiple_of(seg[e, blk], 16), cap)
                rows_x[e, at, :] = jnp.dot(pick, x_b, preferred_element_type=jnp.float32).astype(jnp.bfloat16)
                rows_q[e, at, :] = jnp.dot(pick, q_b, preferred_element_type=jnp.float32).astype(jnp.bfloat16)
            return carry

        lax.fori_loop(0, span, pack, 0)
        for e in range(experts):
            tail = pl.ds(pl.multiple_of(last_row[e, s], 16), TILE)
            rows_x[e, tail, :] = jnp.zeros((TILE, model), jnp.bfloat16)
            rows_q[e, tail, :] = jnp.zeros((TILE, model), jnp.bfloat16)

        @pl.when(s + 1 < nsup)
        def _():
            x_copy(s + 1).start()

        @pl.when(s == 0)
        def _():
            for copy in weights:
                copy.wait()
            if not first:
                for i, (src, dst) in enumerate(zip(prev, sums)):
                    pltpu.make_async_copy(src, dst, sem_a.at[i]).wait()

        def expert(e, carry):
            def tile(i, carry):
                at = pl.ds(pl.multiple_of(i * TILE, TILE), TILE)
                x_t = rows_x[e, at, :]
                q_t = rows_q[e, at, :]
                u = jnp.dot(x_t, wgu[e, :, 0:ff], preferred_element_type=jnp.float32).astype(jnp.bfloat16).astype(jnp.float32)
                v = jnp.dot(x_t, wgu[e, :, ff:2 * ff], preferred_element_type=jnp.float32).astype(jnp.bfloat16).astype(jnp.float32)
                r = jnp.dot(q_t, wdt[e], preferred_element_type=jnp.float32)
                sig = jax.nn.sigmoid(u)
                us = u * sig
                hidden = (us * v).astype(jnp.bfloat16)
                dh[:, 0:ff] = (r * v * sig * (1.0 + u * (1.0 - sig))).astype(jnp.bfloat16)
                dh[:, ff:2 * ff] = (r * us).astype(jnp.bfloat16)
                d_t = dh[...]
                over_rows = (((0,), (0,)), ((), ()))
                acc_gu[e] += lax.dot_general(x_t, d_t, over_rows, preferred_element_type=jnp.float32)
                acc_d[e] += lax.dot_general(hidden, q_t, over_rows, preferred_element_type=jnp.float32)
                rows_x[e, at, :] = jnp.dot(hidden, wd[e], preferred_element_type=jnp.float32).astype(jnp.bfloat16)
                rows_q[e, at, :] = jnp.dot(d_t, wgut[e], preferred_element_type=jnp.float32).astype(jnp.bfloat16)
                return carry

            lax.fori_loop(0, tiles[e, s], tile, 0)
            return carry

        lax.fori_loop(0, experts, expert, 0)

        def unpack(b, carry):
            rows = pl.ds(pl.multiple_of(b * tok, tok), tok)
            blk = s * span + b
            o_slot = lax.rem(blk, 2)

            @pl.when(blk >= 2)
            def _():
                for copy in out_copies(blk - 2, o_slot):
                    copy.wait()

            dy_b = dybuf[slot, rows, :].astype(jnp.float32)
            y_b = gx_b = None
            for e in range(experts):
                at = pl.ds(pl.multiple_of(seg[e, blk], 16), cap)
                hit = lax.broadcasted_iota(jnp.int32, (tok, cap), 1).astype(jnp.float32) == colbuf[slot, rows, experts + e:experts + e + 1]
                put = jnp.where(hit, 1.0, 0.0).astype(jnp.bfloat16)
                o_b = jnp.dot(put, rows_x[e, at, :], preferred_element_type=jnp.float32)
                p_b = jnp.dot(put, rows_q[e, at, :], preferred_element_type=jnp.float32)
                dgbuf[o_slot, :, e:e + 1] = jnp.sum(dy_b * o_b, axis=1, keepdims=True)
                o_b = colbuf[slot, rows, e:e + 1] * o_b
                y_b = o_b if y_b is None else y_b + o_b
                gx_b = p_b if gx_b is None else gx_b + p_b
            outbuf[o_slot, :, 0:model] = y_b
            outbuf[o_slot, :, model:2 * model] = gx_b
            for copy in out_copies(blk, o_slot):
                copy.start()
            return carry

        lax.fori_loop(0, span, unpack, 0)
        return carry

    lax.fori_loop(0, nsup, step, 0)
    outs = [pltpu.make_async_copy(src, dst, sem_a.at[i]) for i, (src, dst) in enumerate(zip(sums, (gg_hbm, gu_hbm, gd_hbm)))]
    for copy in outs:
        copy.start()
    for blk in (nblk - 2, nblk - 1):
        for copy in out_copies(blk, blk % 2):
            copy.wait()
    for copy in outs:
        copy.wait()


def tables(gate):
    micro, nblk, experts, tok = gate.shape
    span = blocks_per_step(nblk)
    gate = jnp.transpose(gate, (0, 2, 1, 3))
    chosen = gate >= 0.0
    before = jnp.triu(jnp.ones((tok, tok), jnp.bfloat16), 1)
    pos = jnp.einsum("mlgt,tu->mlgu", chosen.astype(jnp.bfloat16), before, preferred_element_type=jnp.float32)
    pos = jnp.where(chosen, pos, -1.0)
    count = jnp.sum(chosen.astype(jnp.int32), axis=3)
    room = ((count + 15) // 16 * 16).reshape(micro, experts, nblk // span, span)
    ends = jnp.cumsum(room, axis=3)
    seg = (ends - room).reshape(micro, experts, nblk)
    last_row = ends[..., -1]
    cols = jnp.concatenate([jnp.maximum(gate, 0.0), pos], axis=1).reshape(micro, 2 * experts, nblk * tok)
    cols = jnp.pad(jnp.transpose(cols, (0, 2, 1)), ((0, 0), (0, 0), (0, LANES - 2 * experts)))
    made = (seg, last_row, (last_row + TILE - 1) // TILE, pos.astype(jnp.int32), cols)
    return lax.optimization_barrier([tuple(table[m] for table in made) for m in range(micro)])


def blocks_per_step(nblk):
    return 8 if nblk % 8 == 0 else nblk


def run_experts(made, tokens, weights, prev):
    seg, last_row, tiles, pos, cols = made
    experts, nblk, tok = pos.shape
    model, ff = weights[0].shape[1], weights[1].shape[1]
    cap = tok // 2
    span = blocks_per_step(nblk)
    rows = nblk * tok
    f32, bf16 = jnp.float32, jnp.bfloat16
    packed = span * cap + TILE
    smem, anywhere = pl.BlockSpec(memory_space=pltpu.SMEM), pl.BlockSpec(memory_space=pl.ANY)
    vmem = pl.BlockSpec(memory_space=pltpu.VMEM)
    first = prev is None
    args = [seg, last_row, tiles, pos, tokens, cols, *weights] + ([] if first else list(prev))
    dims = (nblk, span, tok, model, ff, experts, cap)
    return pl.pallas_call(
        functools.partial(expert_kernel, dims, first),
        name="experts_first" if first else "experts_next",
        out_shape=(jax.ShapeDtypeStruct((rows, 2 * model), f32),
                   jax.ShapeDtypeStruct((rows, LANES), f32), jax.ShapeDtypeStruct((experts, model, ff), f32),
                   jax.ShapeDtypeStruct((experts, model, ff), f32), jax.ShapeDtypeStruct((experts, ff, model), f32)),
        in_specs=[smem] * 3 + [vmem] + [anywhere] * (len(args) - 4),
        out_specs=(anywhere,) * 5,
        scratch_shapes=[
            pltpu.VMEM((experts, packed, model), bf16), pltpu.VMEM((experts, packed, model), bf16),
            pltpu.VMEM((experts, model, 2 * ff), bf16), pltpu.VMEM((experts, ff, model), bf16),
            pltpu.VMEM((experts, model, ff), bf16), pltpu.VMEM((experts, 2 * ff, model), bf16),
            pltpu.VMEM((experts, model, 2 * ff), f32), pltpu.VMEM((experts, ff, model), f32),
            pltpu.VMEM((span * tok, model), bf16), pltpu.VMEM((2, span * tok, model), bf16),
            pltpu.VMEM((2, span * tok, LANES), f32),
            pltpu.VMEM((2, tok, 2 * model), f32), pltpu.VMEM((2, tok, LANES), f32),
            pltpu.VMEM((TILE, 2 * ff), bf16),
            pltpu.SemaphoreType.DMA, pltpu.SemaphoreType.DMA((2,)), pltpu.SemaphoreType.DMA((2,)),
            pltpu.SemaphoreType.DMA((4,)), pltpu.SemaphoreType.DMA((3,)),
            pltpu.SemaphoreType.DMA((2,)), pltpu.SemaphoreType.DMA((2,)),
        ],
        compiler_params=pltpu.CompilerParams(vmem_limit_bytes=66 * 1000 * 1000),
        cost_estimate=pl.CostEstimate(flops=18 * rows * model * ff, bytes_accessed=12 * rows * model, transcendentals=rows * ff),
    )(*args)


def solution(mesh):
    group_size = mesh.shape["row"] * mesh.shape["col"] * mesh.shape["core"]
    tok_spec = P(None, ALL_AXES, None)
    w_spec = P(ALL_AXES, None, None)

    def moe_layer(x, route_idx, gates, w_gate, w_up, w_down, grad_y):
        micro, tok = x.shape[0], x.shape[1]
        local = w_gate.shape[0]
        gathered = [lax.all_gather(jnp.stack([x[m], grad_y[m]]), GROUP_AXES, axis=1, tiled=True) for m in range(micro)]
        route_t = jnp.transpose(route_idx, (0, 2, 1))
        gates_t = jnp.transpose(gates, (0, 2, 1))
        hits = route_t[:, :, None, :] == jnp.arange(group_size * local)[None, None, :, None]
        table = jnp.where(jnp.any(hits, axis=1), jnp.sum(jnp.where(hits, gates_t[:, :, None, :], 0.0), axis=1), -1.0)
        made = tables(lax.all_to_all(table.reshape(micro, group_size, local, tok), GROUP_AXES, 1, 1, tiled=True))
        weights = (jnp.concatenate([w_gate, w_up], axis=2), w_down, jnp.transpose(w_down, (0, 2, 1)),
                   jnp.concatenate([jnp.transpose(w_gate, (0, 2, 1)), jnp.transpose(w_up, (0, 2, 1))], axis=1))
        outs_y, outs_dx, outs_dg = [], [], []
        sums = None
        for m in range(micro):
            part, part_dg, *sums = run_experts(made[m], gathered[m], weights, sums)
            whole = lax.psum_scatter(part, GROUP_AXES, scatter_dimension=0, tiled=True).astype(x.dtype)
            outs_y.append(whole[:, :x.shape[2]])
            outs_dx.append(whole[:, x.shape[2]:])
            part_dg = jnp.transpose(part_dg[:, :local].reshape(group_size, tok, local), (0, 2, 1))
            by_expert = lax.all_to_all(part_dg, GROUP_AXES, 0, 0, tiled=True).reshape(group_size * local, tok)
            outs_dg.append(jnp.sum(jnp.where(hits[m], by_expert[None], 0.0), axis=1).T)
        return (jnp.stack(outs_y), jnp.stack(outs_dx), jnp.stack(outs_dg), *sums)

    return jax.shard_map(moe_layer, mesh=mesh, in_specs=(tok_spec, tok_spec, tok_spec, w_spec, w_spec, w_spec, tok_spec), out_specs=(tok_spec, tok_spec, tok_spec, w_spec, w_spec, w_spec), check_vma=False)
```

```python
import functools

import jax
import jax.numpy as jnp
from jax import lax
from jax.experimental import pallas as pl
from jax.experimental.pallas import tpu as pltpu
from jax.sharding import PartitionSpec as P

GROUP_AXES = ("row", "col", "core")
ALL_AXES = ("rep", "row", "col", "core")
TILE = 256
LANES = 128
HALVES = 2


def expert_kernel(dims, first, *refs):
    nblk, span, tok, model, ff, experts, cap = dims
    nsup = nblk // span
    seg, last_row, tiles, pos_rows, tokens, cols_hbm, wgu_hbm, wd_hbm, wdt_hbm, wgut_hbm = refs[:10]
    refs = refs[10:]
    if not first:
        prev, refs = refs[:3], refs[3:]
    out_hbm, dg_hbm, gg_hbm, gu_hbm, gd_hbm = refs[:5]
    (rows_x, rows_q, wgu, wd, wdt, wgut, acc_gu, acc_d, xbuf, dybuf, colbuf, outbuf, dgbuf, dh, sem_x, sem_dy, sem_c,
     sem_w, sem_a, sem_out, sem_dg) = refs[5:]

    def x_copy(s):
        return pltpu.make_async_copy(tokens.at[0, pl.ds(s * span * tok, span * tok)], xbuf, sem_x)

    def dy_copy(s, slot):
        return pltpu.make_async_copy(tokens.at[1, pl.ds(s * span * tok, span * tok)], dybuf.at[slot], sem_dy.at[slot])

    def col_copy(s, slot):
        return pltpu.make_async_copy(cols_hbm.at[pl.ds(s * span * tok, span * tok)], colbuf.at[slot], sem_c.at[slot])

    def out_copies(blk, slot):
        where = pl.ds(blk * tok, tok)
        return (pltpu.make_async_copy(outbuf.at[slot], out_hbm.at[where], sem_out.at[slot]),
                pltpu.make_async_copy(dgbuf.at[slot], dg_hbm.at[where], sem_dg.at[slot]))

    weights = [pltpu.make_async_copy(src, dst, sem_w.at[i])
               for i, (src, dst) in enumerate(((wgu_hbm, wgu), (wd_hbm, wd), (wdt_hbm, wdt), (wgut_hbm, wgut)))]
    sums = (acc_gu.at[:, :, pl.ds(0, ff)], acc_gu.at[:, :, pl.ds(ff, ff)], acc_d)

    x_copy(0).start()
    dy_copy(0, 0).start()
    col_copy(0, 0).start()
    for copy in weights:
        copy.start()
    if first:
        for e in range(experts):
            @pl.loop(0, model // 128)
            def _(i, e=e):
                acc_gu[e, pl.ds(i * 128, 128), :] = jnp.zeros((128, 2 * ff), jnp.float32)

            @pl.loop(0, ff // 128)
            def _(i, e=e):
                acc_d[e, pl.ds(i * 128, 128), :] = jnp.zeros((128, model), jnp.float32)
    else:
        for i, (src, dst) in enumerate(zip(prev, sums)):
            pltpu.make_async_copy(src, dst, sem_a.at[i]).start()

    def step(s, carry):
        slot = lax.rem(s, 2)
        x_copy(s).wait()
        dy_copy(s, slot).wait()
        col_copy(s, slot).wait()

        @pl.when(s + 1 < nsup)
        def _():
            dy_copy(s + 1, 1 - slot).start()
            col_copy(s + 1, 1 - slot).start()

        def pack(b, carry):
            rows = pl.ds(pl.multiple_of(b * tok, tok), tok)
            blk = s * span + b
            x_b = xbuf[rows, :]
            dy_b = dybuf[slot, rows, :].astype(jnp.float32)
            for e in range(experts):
                gate = colbuf[slot, rows, e:e + 1]
                q_b = (gate * dy_b).astype(jnp.bfloat16)
                hit = lax.broadcasted_iota(jnp.int32, (cap, tok), 0) == pos_rows[e, pl.ds(blk, 1), :]
                pick = jnp.where(hit, 1.0, 0.0).astype(jnp.bfloat16)
                at = pl.ds(pl.multiple_of(seg[e, blk], 16), cap)
                rows_x[e, at, :] = jnp.dot(pick, x_b, preferred_element_type=jnp.float32).astype(jnp.bfloat16)
                rows_q[e, at, :] = jnp.dot(pick, q_b, preferred_element_type=jnp.float32).astype(jnp.bfloat16)
            return carry

        lax.fori_loop(0, span, pack, 0)
        for e in range(experts):
            tail = pl.ds(pl.multiple_of(last_row[e, s], 16), TILE)
            rows_x[e, tail, :] = jnp.zeros((TILE, model), jnp.bfloat16)
            rows_q[e, tail, :] = jnp.zeros((TILE, model), jnp.bfloat16)

        @pl.when(s + 1 < nsup)
        def _():
            x_copy(s + 1).start()

        @pl.when(s == 0)
        def _():
            for copy in weights:
                copy.wait()
            if not first:
                for i, (src, dst) in enumerate(zip(prev, sums)):
                    pltpu.make_async_copy(src, dst, sem_a.at[i]).wait()

        def expert(e, carry):
            def tile(i, carry):
                at = pl.ds(pl.multiple_of(i * TILE, TILE), TILE)
                x_t = rows_x[e, at, :]
                q_t = rows_q[e, at, :]
                u = jnp.dot(x_t, wgu[e, :, 0:ff], preferred_element_type=jnp.float32).astype(jnp.bfloat16).astype(jnp.float32)
                v = jnp.dot(x_t, wgu[e, :, ff:2 * ff], preferred_element_type=jnp.float32).astype(jnp.bfloat16).astype(jnp.float32)
                r = jnp.dot(q_t, wdt[e], preferred_element_type=jnp.float32)
                sig = jax.nn.sigmoid(u)
                us = u * sig
                hidden = (us * v).astype(jnp.bfloat16)
                dh[:, 0:ff] = (r * v * sig * (1.0 + u * (1.0 - sig))).astype(jnp.bfloat16)
                dh[:, ff:2 * ff] = (r * us).astype(jnp.bfloat16)
                d_t = dh[...]
                over_rows = (((0,), (0,)), ((), ()))
                acc_gu[e] += lax.dot_general(x_t, d_t, over_rows, preferred_element_type=jnp.float32)
                acc_d[e] += lax.dot_general(hidden, q_t, over_rows, preferred_element_type=jnp.float32)
                rows_x[e, at, :] = jnp.dot(hidden, wd[e], preferred_element_type=jnp.float32).astype(jnp.bfloat16)
                rows_q[e, at, :] = jnp.dot(d_t, wgut[e], preferred_element_type=jnp.float32).astype(jnp.bfloat16)
                return carry

            lax.fori_loop(0, tiles[e, s], tile, 0)
            return carry

        lax.fori_loop(0, experts, expert, 0)

        def unpack(b, carry):
            rows = pl.ds(pl.multiple_of(b * tok, tok), tok)
            blk = s * span + b
            o_slot = lax.rem(blk, 2)

            @pl.when(blk >= 2)
            def _():
                for copy in out_copies(blk - 2, o_slot):
                    copy.wait()

            dy_b = dybuf[slot, rows, :].astype(jnp.float32)
            y_b = gx_b = None
            for e in range(experts):
                at = pl.ds(pl.multiple_of(seg[e, blk], 16), cap)
                hit = lax.broadcasted_iota(jnp.int32, (tok, cap), 1).astype(jnp.float32) == colbuf[slot, rows, experts + e:experts + e + 1]
                put = jnp.where(hit, 1.0, 0.0).astype(jnp.bfloat16)
                o_b = jnp.dot(put, rows_x[e, at, :], preferred_element_type=jnp.float32)
                p_b = jnp.dot(put, rows_q[e, at, :], preferred_element_type=jnp.float32)
                dgbuf[o_slot, :, e:e + 1] = jnp.sum(dy_b * o_b, axis=1, keepdims=True)
                o_b = colbuf[slot, rows, e:e + 1] * o_b
                y_b = o_b if y_b is None else y_b + o_b
                gx_b = p_b if gx_b is None else gx_b + p_b
            outbuf[o_slot, :, 0:model] = y_b
            outbuf[o_slot, :, model:2 * model] = gx_b
            for copy in out_copies(blk, o_slot):
                copy.start()
            return carry

        lax.fori_loop(0, span, unpack, 0)
        return carry

    lax.fori_loop(0, nsup, step, 0)
    outs = [pltpu.make_async_copy(src, dst, sem_a.at[i]) for i, (src, dst) in enumerate(zip(sums, (gg_hbm, gu_hbm, gd_hbm)))]
    for copy in outs:
        copy.start()
    for blk in (nblk - 2, nblk - 1):
        for copy in out_copies(blk, blk % 2):
            copy.wait()
    for copy in outs:
        copy.wait()


def tables(gate):
    micro, nblk, experts, tok = gate.shape
    span = blocks_per_step(nblk, tok)
    gate = jnp.transpose(gate, (0, 2, 1, 3))
    chosen = gate >= 0.0
    before = jnp.triu(jnp.ones((tok, tok), jnp.bfloat16), 1)
    pos = jnp.einsum("mlgt,tu->mlgu", chosen.astype(jnp.bfloat16), before, preferred_element_type=jnp.float32)
    pos = jnp.where(chosen, pos, -1.0)
    count = jnp.sum(chosen.astype(jnp.int32), axis=3)
    room = ((count + 15) // 16 * 16).reshape(micro, experts, nblk // span, span)
    ends = jnp.cumsum(room, axis=3)
    seg = (ends - room).reshape(micro, experts, nblk)
    last_row = ends[..., -1]
    cols = jnp.concatenate([jnp.maximum(gate, 0.0), pos], axis=1).reshape(micro, 2 * experts, nblk * tok)
    cols = jnp.pad(jnp.transpose(cols, (0, 2, 1)), ((0, 0), (0, 0), (0, LANES - 2 * experts)))
    made = (seg, last_row, (last_row + TILE - 1) // TILE, pos.astype(jnp.int32), cols)
    return lax.optimization_barrier([tuple(table[m] for table in made) for m in range(micro)])


def blocks_per_step(nblk, tok):
    span = 2048 // tok
    return span if nblk % span == 0 else nblk


def run_experts(made, tokens, weights, prev, cap):
    seg, last_row, tiles, pos, cols = made
    experts, nblk, tok = pos.shape
    model, ff = weights[0].shape[1], weights[1].shape[1]
    span = blocks_per_step(nblk, tok)
    rows = nblk * tok
    f32, bf16 = jnp.float32, jnp.bfloat16
    packed = span * cap + TILE
    smem, anywhere = pl.BlockSpec(memory_space=pltpu.SMEM), pl.BlockSpec(memory_space=pl.ANY)
    vmem = pl.BlockSpec(memory_space=pltpu.VMEM)
    first = prev is None
    args = [seg, last_row, tiles, pos, tokens, cols, *weights] + ([] if first else list(prev))
    dims = (nblk, span, tok, model, ff, experts, cap)
    return pl.pallas_call(
        functools.partial(expert_kernel, dims, first),
        name="experts_first" if first else "experts_next",
        out_shape=(jax.ShapeDtypeStruct((rows, 2 * model), f32),
                   jax.ShapeDtypeStruct((rows, LANES), f32), jax.ShapeDtypeStruct((experts, model, ff), f32),
                   jax.ShapeDtypeStruct((experts, model, ff), f32), jax.ShapeDtypeStruct((experts, ff, model), f32)),
        in_specs=[smem] * 3 + [vmem] + [anywhere] * (len(args) - 4),
        out_specs=(anywhere,) * 5,
        scratch_shapes=[
            pltpu.VMEM((experts, packed, model), bf16), pltpu.VMEM((experts, packed, model), bf16),
            pltpu.VMEM((experts, model, 2 * ff), bf16), pltpu.VMEM((experts, ff, model), bf16),
            pltpu.VMEM((experts, model, ff), bf16), pltpu.VMEM((experts, 2 * ff, model), bf16),
            pltpu.VMEM((experts, model, 2 * ff), f32), pltpu.VMEM((experts, ff, model), f32),
            pltpu.VMEM((span * tok, model), bf16), pltpu.VMEM((2, span * tok, model), bf16),
            pltpu.VMEM((2, span * tok, LANES), f32),
            pltpu.VMEM((2, tok, 2 * model), f32), pltpu.VMEM((2, tok, LANES), f32),
            pltpu.VMEM((TILE, 2 * ff), bf16),
            pltpu.SemaphoreType.DMA, pltpu.SemaphoreType.DMA((2,)), pltpu.SemaphoreType.DMA((2,)),
            pltpu.SemaphoreType.DMA((4,)), pltpu.SemaphoreType.DMA((3,)),
            pltpu.SemaphoreType.DMA((2,)), pltpu.SemaphoreType.DMA((2,)),
        ],
        compiler_params=pltpu.CompilerParams(vmem_limit_bytes=66 * 1000 * 1000),
        cost_estimate=pl.CostEstimate(flops=18 * rows * model * ff, bytes_accessed=12 * rows * model, transcendentals=rows * ff),
    )(*args)


def solution(mesh):
    group_size = mesh.shape["row"] * mesh.shape["col"] * mesh.shape["core"]
    tok_spec = P(None, ALL_AXES, None)
    w_spec = P(ALL_AXES, None, None)

    def moe_layer(x, route_idx, gates, w_gate, w_up, w_down, grad_y):
        micro, tok = x.shape[0], x.shape[1]
        local = w_gate.shape[0]
        cap, half = tok // 2, tok // HALVES
        pieces = [(m, slice(h * half, (h + 1) * half)) for m in range(micro) for h in range(HALVES)]
        gathered = [lax.all_gather(jnp.stack([x[m, part], grad_y[m, part]]), GROUP_AXES, axis=1, tiled=True) for m, part in pieces]
        route_t = jnp.transpose(route_idx, (0, 2, 1))
        gates_t = jnp.transpose(gates, (0, 2, 1))
        hits = route_t[:, :, None, :] == jnp.arange(group_size * local)[None, None, :, None]
        table = jnp.where(jnp.any(hits, axis=1), jnp.sum(jnp.where(hits, gates_t[:, :, None, :], 0.0), axis=1), -1.0)
        table = lax.all_to_all(table.reshape(micro, group_size, local, tok), GROUP_AXES, 1, 1, tiled=True)
        table = jnp.moveaxis(table.reshape(micro, group_size, local, HALVES, half), 3, 1)
        made = tables(table.reshape(micro * HALVES, group_size, local, half))
        weights = (jnp.concatenate([w_gate, w_up], axis=2), w_down, jnp.transpose(w_down, (0, 2, 1)),
                   jnp.concatenate([jnp.transpose(w_gate, (0, 2, 1)), jnp.transpose(w_up, (0, 2, 1))], axis=1))
        outs, gate_parts = [], []
        sums = None
        for piece in range(len(pieces)):
            part, part_dg, *sums = run_experts(made[piece], gathered[piece], weights, sums, cap)
            outs.append(lax.psum_scatter(part, GROUP_AXES, scatter_dimension=0, tiled=True).astype(x.dtype))
            gate_parts.append(part_dg[:, :local].reshape(group_size, half, local))
        both = jnp.stack(outs).reshape(micro, tok, 2 * x.shape[2])
        gate_parts = jnp.stack(gate_parts).reshape(micro, HALVES, group_size, half, local)
        gate_parts = jnp.transpose(gate_parts, (2, 0, 4, 1, 3)).reshape(group_size, micro, local, tok)
        by_expert = lax.all_to_all(gate_parts, GROUP_AXES, 0, 0, tiled=True)
        by_expert = jnp.swapaxes(by_expert, 0, 1).reshape(micro, 1, group_size * local, tok)
        grad_gates = jnp.transpose(jnp.sum(jnp.where(hits, by_expert, 0.0), axis=2), (0, 2, 1))
        return (both[:, :, :x.shape[2]], both[:, :, x.shape[2]:], grad_gates, *sums)

    return jax.shard_map(moe_layer, mesh=mesh, in_specs=(tok_spec, tok_spec, tok_spec, w_spec, w_spec, w_spec, tok_spec), out_specs=(tok_spec, tok_spec, tok_spec, w_spec, w_spec, w_spec), check_vma=False)
```
